256 devices in a mesh: scene: 4 (over x, y), az: 64 (over z, core).
Axes of the slice: x: 2, y: 2, z: 32, core: 2. Of those that a mesh axis runs over, the one named last changes fastest.
The devices are a block of a 4x8x32 slice.
Arguments:
- secondary: bfloat16 [2, 16384, 12288], P(None, ('scene', 'az')), parts along dimension 1, may hold values from -6 to 6
- line_valid: int32 [16384], P(('scene', 'az')), parts along dimension 0, may hold values 0 or 1
- first_valid: int32 [16384], P(('scene', 'az')), parts along dimension 0, may hold values from 0 to 3071
- last_valid: int32 [16384], P(('scene', 'az')), parts along dimension 0, may hold values from 9216 to 12288
- az_coef: float32 [3, 16384], P(None, ('scene', 'az')), parts along dimension 1, may hold values from -0.33 to 0.33
- az_base: int32 [16384], P(('scene', 'az')), parts along dimension 0, may hold values from -3 to 3
- rg_base: int32 [16384], P(('scene', 'az')), parts along dimension 0, may hold values from -8 to 8
- rg_coef: float32 [16], P('scene'), parts along dimension 0, may hold values from -3 to 3
- block_dest: int32 [16384], P(('scene', 'az')), parts along dimension 0, may hold values from 0 to 4095, as said below
Outputs:
- coreg: bfloat16 [2, 16384, 12288], P(None, ('scene', 'az')), parts along dimension 1
- mean_power: float32 [4], P('scene'), parts along dimension 0
- valid_share: float32 [4], P('scene'), parts along dimension 0
The draws below stay inside these ranges and needn't reach their ends.
There are 4 independent parts, one for each index of `scene`. The reference program is written for one: setup_inputs(seed, part) draws one part's arguments, and reference() takes and returns one part's arrays. A program takes and returns all parts, laid end to end along the dimension named above; each array names one. Nothing has to cross between parts.
Inputs may be any that keep to these rules, and one draw needn't show every extreme that they name: `block_dest`: A permutation of 0 to 4095. The 64 line blocks of each device of az take exactly one place on every device of az, itself included (place // 64 runs over all devices).
All inputs are finite; a program needn't handle non-finite values. No bound on the sum of `line_valid` on one device may be relied on, other than what follows from the above.
Results may differ from the reference program's by a relative error of at most 0.0066.
Values may be sent and summed in bfloat16 or wider, within the bound.
No kernel may reach another device: no remote copies, remote signals or barrier semaphores. Data moves between devices by JAX's collectives and lax.ppermute only.
A program may use at most 128 MiB of HBM per device.

```python
import jax
import jax.numpy as jnp
from jax import lax

LINES = 1
RG = 12288
ABASE = 3
RBMAX = 8
HALO = 7
BLK_DEV = 64
AZ = 4096
NBLK = 4096


def draw_secondary(key, part):
    first_key, second_key = jax.random.split(key)
    values = jax.random.normal(first_key, (2, AZ, RG), jnp.float32)
    return jnp.clip(values, -6.0, 6.0).astype(jnp.bfloat16)


def draw_block_dest(key, part):
    blocks = BLK_DEV
    first_key, second_key = jax.random.split(key)
    offsets = jax.vmap(lambda inner_key: jax.random.permutation(inner_key, blocks))(jax.random.split(first_key, blocks))
    places = jax.vmap(lambda inner_key: jax.random.permutation(inner_key, blocks))(jax.random.split(second_key, blocks))
    source = jnp.broadcast_to(jnp.arange(blocks)[:, None], (blocks, blocks))
    target = (source + offsets) % blocks
    slot_at = places[target, source]
    return (target * blocks + slot_at).reshape(-1).astype(jnp.int32)


def touch_ends(array, stream_key, least, top_value):
    dims = array.shape
    index_at = [jax.random.randint(jax.random.fold_in(stream_key, axis), (), 0, dims[axis]) for axis in range(len(dims))]
    array = array.at[tuple(index_at)].set(least)
    longest = dims.index(max(dims))
    index_at[longest] = (index_at[longest] + 1) % dims[longest]
    return array.at[tuple(index_at)].set(top_value)


def block_levels(own_key, dims, cuts, low, largest):
    factor_of, own = 1.0, jax.random.fold_in(own_key, 6)
    for dim, parts in cuts:
        draws = jnp.exp(jax.random.uniform(jax.random.fold_in(own, dim), (parts,), jnp.float32, low / len(cuts), largest / len(cuts)))
        factor_of = factor_of * jnp.repeat(draws, dims[dim] // parts).reshape([-1 if axis == dim else 1 for axis in range(len(dims))])
    return factor_of


def setup_inputs(seed: int = 0, part: int = 0) -> dict:
    key_list = jax.random.split(jax.random.key(seed), 10)
    own_keys = jax.random.split(jax.random.fold_in(key_list[9], part), 10)
    return {
        "secondary": draw_secondary(jax.random.fold_in(jax.random.fold_in(key_list[9], part), 71), part),
        "line_valid": touch_ends((jax.random.randint(own_keys[1], (AZ,), 0, 4) < 3).astype(jnp.int32), jax.random.fold_in(own_keys[1], 1), 0, 1),
        "first_valid": touch_ends(jax.random.randint(own_keys[2], (AZ,), 0, RG // 4), jax.random.fold_in(own_keys[2], 1), 0, (RG // 4) - 1).astype(jnp.int32),
        "last_valid": touch_ends(jax.random.randint(own_keys[3], (AZ,), RG - RG // 4, RG + 1), jax.random.fold_in(own_keys[3], 1), RG - RG // 4, RG).astype(jnp.int32),
        "az_coef": jnp.clip(jax.random.uniform(own_keys[4], (3, NBLK), jnp.float32, -0.33, 0.33) * block_levels(own_keys[4], (3, NBLK), ((1, 64),), -0.4, 0.0), -0.33, 0.33),
        "az_base": touch_ends(jax.random.randint(own_keys[5], (NBLK,), -ABASE, ABASE + 1), jax.random.fold_in(own_keys[5], 1), -ABASE, ABASE).astype(jnp.int32),
        "rg_base": touch_ends(jax.random.randint(own_keys[6], (NBLK,), -RBMAX, RBMAX + 1), jax.random.fold_in(own_keys[6], 1), -RBMAX, RBMAX).astype(jnp.int32),
        "rg_coef": jnp.clip(jax.random.uniform(own_keys[7], (4,), jnp.float32, -3.0, 3.0), -3.0, 3.0),
        "block_dest": draw_block_dest(jax.random.fold_in(jax.random.fold_in(key_list[9], part), 71), part),
    }


def sinc_taper(distance):
    in_reach = jnp.abs(distance) < 4.0
    shaped = jnp.sinc(distance) * (0.5 + 0.5 * jnp.cos(jnp.pi * distance / 4.0))
    return jnp.where(in_reach, shaped, jnp.zeros_like(distance))

def tap_weights(az_coef, line_count):
    position = (jnp.arange(line_count, dtype=jnp.float32) + 0.5) / line_count
    fraction = az_coef[0][:, None] + az_coef[1][:, None] * position + az_coef[2][:, None] * position * position
    tap_offsets = jnp.arange(9, dtype=jnp.float32) - 4.0
    return sinc_taper(tap_offsets[None, None, :] - fraction[:, :, None]).astype(jnp.bfloat16)

def range_tiles(rg_coef, col_count):
    tile_total = col_count // 128
    col_index = jnp.arange(col_count, dtype=jnp.float32)
    along = (col_index + 0.5) / col_count
    offsets = rg_coef[0] + rg_coef[1] * along + rg_coef[2] * along * along + rg_coef[3] * along * along * along
    offsets = offsets.reshape(tile_total, 128)
    inner = jnp.arange(128, dtype=jnp.float32)
    tile_gaps = (jnp.arange(3, dtype=jnp.float32) - 1.0) * 128.0
    distance = tile_gaps[:, None, None, None] + inner[None, None, :, None] - inner[None, None, None, :] - offsets[None, :, None, :]
    return sinc_taper(distance).astype(jnp.bfloat16)

def resample(windows, weights, kernel):
    line_count = weights.shape[1]
    summed = jnp.zeros(windows.shape[:2] + (line_count, windows.shape[3]), jnp.float32)
    for tap_index in range(9):
        summed = summed + weights[:, None, :, tap_index, None].astype(jnp.float32) * windows[:, :, tap_index:tap_index + line_count, :].astype(jnp.float32)
    azimuthal = summed.astype(jnp.bfloat16)
    col_count = azimuthal.shape[3]
    tile_total = col_count // 128
    tiled_rows = azimuthal.reshape(azimuthal.shape[:3] + (tile_total, 128))
    padded = jnp.pad(tiled_rows, ((0, 0), (0, 0), (0, 0), (1, 1), (0, 0)))
    ranged = jnp.zeros(tiled_rows.shape, jnp.float32)
    for shift_tile in range(3):
        ranged = ranged + jnp.einsum('bclti,tij->bcltj', padded[:, :, :, shift_tile:shift_tile + tile_total].astype(jnp.float32), kernel[shift_tile].astype(jnp.float32))
    return ranged.reshape(azimuthal.shape).astype(jnp.bfloat16)

def reference(secondary, line_valid, first_valid, last_valid, az_coef, az_base, rg_base, rg_coef, block_dest):
    col_index = jnp.arange(RG, dtype=jnp.int32)
    kept_mask = (line_valid[:, None] > 0) & (col_index[None, :] >= first_valid[:, None]) & (col_index[None, :] < last_valid[:, None])
    masked = jnp.where(kept_mask[None], secondary, jnp.zeros((), jnp.bfloat16))
    valid_total = jnp.sum(kept_mask.astype(jnp.int32)).astype(jnp.float32)
    padded = jnp.pad(masked, ((0, 0), (HALO, HALO), (RBMAX, RBMAX)))
    weights = tap_weights(az_coef, LINES)
    kernel = range_tiles(rg_coef, RG)
    row_starts = (jnp.arange(NBLK, dtype=jnp.int32) * LINES + az_base - 4 + HALO).astype(jnp.int32)
    col_starts = (RBMAX + rg_base).astype(jnp.int32)

    def one_group(group_index):
        first_block = (group_index * BLK_DEV).astype(jnp.int32)
        rows_here = lax.dynamic_slice_in_dim(row_starts, first_block, BLK_DEV)
        cols_here = lax.dynamic_slice_in_dim(col_starts, first_block, BLK_DEV)
        windows = jax.vmap(lambda rows_at, cols_at: lax.dynamic_slice(padded, (jnp.int32(0), rows_at, cols_at), (2, LINES + 8, RG)))(rows_here, cols_here)
        group_weights = lax.dynamic_slice_in_dim(weights, first_block, BLK_DEV)
        return resample(windows, group_weights, kernel)
    resampled_groups = lax.map(one_group, jnp.arange(NBLK // BLK_DEV, dtype=jnp.int32))
    resampled = resampled_groups.reshape(NBLK, 2, LINES, RG)
    total_power = jnp.sum(jnp.square(resampled.astype(jnp.float32)))
    mean_power = total_power / jnp.maximum(valid_total, 1.0)
    power_gain = lax.rsqrt(mean_power + 0.5)
    scaled = (resampled.astype(jnp.float32) * power_gain).astype(jnp.bfloat16)
    placed = jnp.zeros_like(scaled).at[block_dest].set(scaled)
    coreg = jnp.moveaxis(placed, 1, 0).reshape(2, AZ, RG)
    valid_share = valid_total / (AZ * RG)
    return (coreg, mean_power.reshape(1), valid_share.reshape(1))
```

```python
import functools
import math

import jax
import jax.numpy as jnp
from jax import lax
from jax.experimental import pallas as pl
from jax.experimental.pallas import tpu as pltpu
from jax.sharding import PartitionSpec as P


EDGE = 8
TAPS = 9
LANES = 128
PAIR = 2 * LANES
MAIN_TILES = 24
UNROLL = 8
TABLE_TILES = 8
PLACE_TILES = 32
EDGE_CHUNKS = 8


def sinc_taper(distance):
    in_reach = jnp.abs(distance) < 4.0
    turn = jnp.pi * distance
    ratio = jnp.where(distance == 0.0, 1.0, jnp.sin(turn) / jnp.where(distance == 0.0, 1.0, turn))
    shaped = ratio * (0.5 + 0.5 * jnp.cos(jnp.pi * distance / 4.0))
    return jnp.where(in_reach, shaped, jnp.zeros_like(distance))


def shift_list(chips):
    half = chips // 2
    rising = [k for k in (3, 5, 8, 13) if k < half]
    falling = [k for k in range(half - 1, 0, -1) if k not in rising]
    return [s * k for k in rising + falling for s in (1, -1)]


def chip_pairs(chips, shift):
    return [(2 * z + c, 2 * ((z + shift) % chips) + c) for z in range(chips) for c in range(2)]


def prepare_body(
    pos_ref, lines_ref, coef_ref, az_ref, rg_ref, dest_ref, valid_ref, first_ref, last_ref, meta_ref, edge_ref
):
    cols = lines_ref.shape[2]
    count = dest_ref.shape[1]
    low = jnp.where(valid_ref[...] > 0, first_ref[...], 2 * cols)
    high = last_ref[...]
    meta_ref[...] = jnp.zeros(meta_ref.shape, jnp.float32)
    meta_ref[0:3, :] = coef_ref[...]
    for row, value in enumerate((az_ref[...], rg_ref[...], dest_ref[...], low, high)):
        meta_ref[3 + row : 4 + row, :] = value.astype(jnp.float32)
    begin = pos_ref[1] * (count - EDGE)
    here = lax.broadcasted_iota(jnp.int32, (EDGE, count), 1) == lax.broadcasted_iota(jnp.int32, (EDGE, count), 0) + begin

    def upright(values):
        spread = jnp.where(here, values.astype(jnp.float32), 0.0)
        return jnp.sum(spread, axis=1, keepdims=True).astype(jnp.int32)

    low_at, high_at = upright(low), upright(high)
    width = cols // EDGE_CHUNKS
    for chunk in range(EDGE_CHUNKS):
        at = slice(chunk * width, (chunk + 1) * width)
        column = lax.broadcasted_iota(jnp.int32, (EDGE, width), 1) + chunk * width
        keep = (column >= low_at) & (column < high_at)
        for part in range(2):
            edge_ref[part, :, at] = jnp.where(keep, lines_ref[part, :, at].astype(jnp.float32), 0.0).astype(jnp.bfloat16)


def prepare_call(pos, secondary, az_coef, *vectors):
    lines, cols = secondary.shape[1:]
    flat = pl.BlockSpec((1, lines), lambda i, pos: (0, 0))
    return pl.pallas_call(
        prepare_body,
        grid_spec=pltpu.PrefetchScalarGridSpec(
            num_scalar_prefetch=1,
            grid=(1,),
            in_specs=[
                pl.BlockSpec((2, EDGE, cols), lambda i, pos: (0, pos[1] * (lines // EDGE - 1), 0)),
                pl.BlockSpec((3, lines), lambda i, pos: (0, 0)),
            ]
            + [flat] * len(vectors),
            out_specs=[
                pl.BlockSpec((16, lines), lambda i, pos: (0, 0)),
                pl.BlockSpec((2, EDGE, cols), lambda i, pos: (0, 0, 0)),
            ],
        ),
        out_shape=[
            jax.ShapeDtypeStruct((16, lines), jnp.float32),
            jax.ShapeDtypeStruct((2, EDGE, cols), jnp.bfloat16),
        ],
        name="prepare",
    )(pos, secondary, az_coef, *[v.reshape(1, lines) for v in vectors])


def table_body(cols, coef_ref, out_ref, taps_ref, whole_ref):
    step = pl.program_id(0)
    tiles = cols // LANES

    @pl.when(step == 0)
    def _():
        shape = (tiles, LANES)
        column = lax.broadcasted_iota(jnp.int32, shape, 0) * LANES + lax.broadcasted_iota(jnp.int32, shape, 1)
        v = (column.astype(jnp.float32) + 0.5) / cols
        offsets = coef_ref[0] + coef_ref[1] * v + coef_ref[2] * v * v + coef_ref[3] * v * v * v
        whole = jnp.round(offsets)
        part = offsets - whole
        whole_ref[...] = whole
        sine = jnp.sin(jnp.pi * part)
        cosine4 = jnp.cos(jnp.pi / 4.0 * part)
        sine4 = jnp.sin(jnp.pi / 4.0 * part)
        for k in range(TAPS):
            m = k - 4
            x = m - part
            turn = jnp.pi * x
            lifted = sine if m % 2 else -sine
            ratio = jnp.where(x == 0.0, 1.0, lifted / jnp.where(x == 0.0, 1.0, turn))
            taper = 0.5 + 0.5 * (math.cos(math.pi * m / 4) * cosine4 + math.sin(math.pi * m / 4) * sine4)
            value = jnp.where(jnp.abs(x) < 4.0, ratio * taper, 0.0)
            taps_ref[k] = value

    gap = (lax.broadcasted_iota(jnp.int32, (16, LANES), 0) - lax.broadcasted_iota(jnp.int32, (16, LANES), 1)).astype(jnp.float32)
    blank = jnp.zeros((16, LANES), jnp.bfloat16)
    pieces = [(16 * g, 16 * g) for g in range(8)] + [(LANES, LANES), (2 * LANES - 16, -16)]
    for tile in range(TABLE_TILES):
        at = pl.ds(step * TABLE_TILES + tile, 1)
        near = (gap - whole_ref[at, :]).astype(jnp.bfloat16)
        taps = [jnp.broadcast_to(taps_ref[k, at, :], (16, LANES)).astype(jnp.bfloat16) for k in range(TAPS)]
        for row, distance in pieces:
            total = blank
            for k in range(TAPS):
                total = jnp.where(near == jnp.bfloat16(k - 4 - distance), taps[k], total)
            out_ref[tile, row : row + 16, :] = total
        for g in range(1, 7):
            out_ref[tile, LANES + 16 * g : LANES + 16 * g + 16, :] = blank


def table_call(coef, cols):
    tiles = cols // LANES
    return pl.pallas_call(
        functools.partial(table_body, cols),
        grid=(tiles // TABLE_TILES,),
        in_specs=[pl.BlockSpec(memory_space=pltpu.SMEM)],
        out_specs=pl.BlockSpec((TABLE_TILES, PAIR, LANES), lambda i: (i, 0, 0)),
        out_shape=jax.ShapeDtypeStruct((tiles, PAIR, LANES), jnp.bfloat16),
        scratch_shapes=[pltpu.VMEM((TAPS, tiles, LANES), jnp.float32), pltpu.VMEM((tiles, LANES), jnp.float32)],
        name="range_table",
    )(coef)


def plan(chips, pos_ref, meta_ref, meta_sib_ref, lhs_ref, lhs_edge_ref, marks_ref):
    chip, core = pos_ref[0], pos_ref[1]
    lines = meta_ref.shape[1]
    count = 2 * lines
    row = lax.broadcasted_iota(jnp.int32, (count, lines), 0)
    turn = row // 4
    shift = jnp.where(turn == chips - 1, chips // 2, 0)
    for at, distance in enumerate(shift_list(chips)):
        shift = jnp.where(turn == at + 1, distance, shift)
    goal = chip + shift
    goal = 2 * jnp.where(goal < 0, goal + chips, jnp.where(goal >= chips, goal - chips, goal)) + core
    from_sib = (row // 2) % 2 == 1
    line = lax.broadcasted_iota(jnp.int32, (count, lines), 1)
    tap = lax.broadcasted_iota(jnp.int32, (16, lines), 0)
    along = lax.broadcasted_iota(jnp.int32, (16, lines), 1)
    picked = None
    for source, (ref, home) in enumerate(((meta_ref, core), (meta_sib_ref, 1 - core))):
        fraction = ref[0:1, :] + ref[1:2, :] * 0.5 + ref[2:3, :] * 0.5 * 0.5
        features = sinc_taper((tap - 4).astype(jnp.float32) - fraction)
        start = (along + home * lines - 4).astype(jnp.float32) + ref[3:4, :]
        features = jnp.where(tap < TAPS, features, jnp.where(tap == TAPS, start, ref[4:5, :]))
        owner = ref[5:6, :].astype(jnp.int32) // lines
        chosen = (owner == goal) & (from_sib if source else ~from_sib)
        found = lax.dot_general(
            jnp.where(chosen, 1.0, 0.0).astype(jnp.bfloat16),
            features.astype(jnp.bfloat16),
            (((1,), (1,)), ((), ())),
            preferred_element_type=jnp.float32,
        )
        picked = found if picked is None else picked + found
    begin = picked[:, TAPS : TAPS + 1]

    def band(coordinate, part):
        row_part = lax.broadcasted_iota(jnp.int32, part.shape, 0) % 2
        step = jnp.where(part == row_part, coordinate.astype(jnp.float32) - begin, -1.0)
        total = jnp.zeros(step.shape, jnp.float32)
        for k in range(TAPS):
            total = jnp.where(step == k, picked[:, k : k + 1], total)
        return total.astype(jnp.bfloat16)

    lane = lax.broadcasted_iota(jnp.int32, (count, count), 1)
    lhs_ref[:, 0:count] = band(lane % lines + core * lines, lane // lines)
    lhs_ref[:, count : 2 * count] = band(lane % lines + (1 - core) * lines, lane // lines)
    slot = lax.broadcasted_iota(jnp.int32, (count, 4 * EDGE), 1)
    high = (slot // (2 * EDGE) + core) % 2 == 1
    coordinate = slot % EDGE + jnp.where(high, 2 * lines, -EDGE)
    lhs_edge_ref[...] = band(coordinate, slot // EDGE % 2)

    level = line == row % lines
    for at, (ref, which) in enumerate(((meta_ref, 6), (meta_ref, 7), (meta_sib_ref, 6), (meta_sib_ref, 7))):
        upright = jnp.sum(jnp.where(level, ref[which : which + 1, :], 0.0), axis=1, keepdims=True)
        marks_ref[at] = jnp.broadcast_to(upright, (count, LANES)).astype(jnp.int32)
    marks_ref[4] = jnp.broadcast_to(picked[:, TAPS + 1 : TAPS + 2], (count, LANES)).astype(jnp.int32)


def filter_body(
    chips, steps, outs, pos_ref, meta_ref, meta_sib_ref, own_ref, sib_ref, near_ref, far_ref, table_ref, *rest
):
    out_refs, power_ref = rest[:outs], rest[outs]
    turned_ref, lhs_ref, lhs_edge_ref, marks_ref, squares_ref = rest[outs + 1 :]
    step = pl.program_id(0)
    lines = own_ref.shape[1]
    count = 2 * lines
    tiles = steps * MAIN_TILES

    @pl.when(step == 0)
    def _():
        plan(chips, pos_ref, meta_ref, meta_sib_ref, lhs_ref, lhs_edge_ref, marks_ref)
        zeros = jnp.zeros((count, LANES), jnp.float32)
        for row in (0, 1, tiles + 2, tiles + 3):
            turned_ref[row] = zeros
        squares_ref[...] = zeros

    lane = lax.broadcasted_iota(jnp.int32, (count, LANES), 1)
    source = lane + marks_ref[4]
    before = source < 0
    after = source >= LANES
    wrapped = source & (LANES - 1)

    @pl.when(step < steps)
    def _():
        def run(turn, _):
            for pair in range(UNROLL // 2):
                tile = turn * UNROLL + 2 * pair
                here = step * MAIN_TILES + tile
                both = pl.ds(pl.multiple_of(tile * LANES, PAIR), PAIR)

                def kept(ref, low, high):
                    values = ref[:, :, both].reshape(count, PAIR).astype(jnp.float32)
                    halves = []
                    for half in range(2):
                        column = lane + (here + half) * LANES
                        inside = (column >= marks_ref[low]) & (column < marks_ref[high])
                        value = values[:, half * LANES : (half + 1) * LANES]
                        halves.append(jnp.where(inside, value, 0.0).astype(jnp.bfloat16))
                    return jnp.concatenate(halves, axis=1)

                data = jnp.concatenate([kept(own_ref, 0, 1), kept(sib_ref, 2, 3)], axis=0)
                edges = jnp.concatenate(
                    [near_ref[:, :, both].reshape(2 * EDGE, PAIR), far_ref[:, :, both].reshape(2 * EDGE, PAIR)], axis=0
                )
                summed = jnp.dot(lhs_ref[...], data, preferred_element_type=jnp.float32)
                summed += jnp.dot(lhs_edge_ref[...], edges, preferred_element_type=jnp.float32)
                rounded = summed.astype(jnp.bfloat16).astype(jnp.float32)
                for half in range(2):
                    turned_ref[here + half + 2] = jnp.take_along_axis(
                        rounded[:, half * LANES : (half + 1) * LANES], wrapped, axis=1, mode="promise_in_bounds"
                    )
            return None

        lax.fori_loop(0, MAIN_TILES // UNROLL, run, None)

    def move(tile):
        here = jnp.where(before, turned_ref[tile + 1], jnp.where(after, turned_ref[tile + 3], turned_ref[tile + 2]))
        return jnp.where((tile >= 0) & (tile < tiles), here, 0.0)

    @pl.when(step > 0)
    def _():
        left = lane < LANES // 2
        first = (step - 1) * MAIN_TILES

        def run(turn, carry):
            squares, previous, middle = carry
            for inner in range(UNROLL):
                tile = turn * UNROLL + inner
                at = pl.ds(pl.multiple_of(tile * LANES, LANES), LANES)
                following = move(first + tile + 1)
                window = jnp.concatenate([middle, jnp.where(left, following, previous)], axis=1).astype(jnp.bfloat16)
                done = jnp.dot(window, table_ref[tile], preferred_element_type=jnp.float32).astype(jnp.bfloat16)
                wide = done.astype(jnp.float32)
                squares += wide * wide
                row = 0
                for ref in out_refs:
                    ref[:, at] = wide[row : row + ref.shape[0]].astype(jnp.bfloat16)
                    row += ref.shape[0]
                previous, middle = middle, following
            return squares, previous, middle

        start = (squares_ref[...], move(first - 1), move(first))
        squares_ref[...] = lax.fori_loop(0, MAIN_TILES // UNROLL, run, start)[0]

    @pl.when(step == steps)
    def _():
        power_ref[0] = jnp.sum(squares_ref[...])


def filter_call(chips, pos, meta, meta_sib, own, sib, near, far, table, row_counts):
    lines, cols = own.shape[1:]
    count = 2 * lines
    tiles = cols // LANES
    steps = tiles // MAIN_TILES
    block = MAIN_TILES * LANES

    def incoming(i):
        return (0, 0, jnp.minimum(i, steps - 1))

    def outgoing(i):
        return (0, jnp.maximum(i - 1, 0))

    smem = pl.BlockSpec(memory_space=pltpu.SMEM)
    return pl.pallas_call(
        functools.partial(filter_body, chips, steps, len(row_counts)),
        grid=(steps + 1,),
        in_specs=[
            smem,
            pl.BlockSpec(meta.shape, lambda i: (0, 0)),
            pl.BlockSpec(meta.shape, lambda i: (0, 0)),
            pl.BlockSpec((2, lines, block), incoming),
            pl.BlockSpec((2, lines, block), incoming),
            pl.BlockSpec((2, EDGE, block), incoming),
            pl.BlockSpec((2, EDGE, block), incoming),
            pl.BlockSpec((MAIN_TILES, PAIR, LANES), lambda i: (jnp.maximum(i - 1, 0), 0, 0)),
        ],
        out_specs=[pl.BlockSpec((rows, block), outgoing) for rows in row_counts] + [smem],
        out_shape=[jax.ShapeDtypeStruct((rows, cols), jnp.bfloat16) for rows in row_counts]
        + [jax.ShapeDtypeStruct((1,), jnp.float32)],
        scratch_shapes=[
            pltpu.VMEM((tiles + 4, count, LANES), jnp.float32),
            pltpu.VMEM((count, 2 * count), jnp.bfloat16),
            pltpu.VMEM((count, 4 * EDGE), jnp.bfloat16),
            pltpu.VMEM((5, count, LANES), jnp.int32),
            pltpu.VMEM((count, LANES), jnp.float32),
        ],
        name="line_filter",
    )(pos, meta, meta_sib, own, sib, near, far, table)


def place_body(ins, gain_ref, arrange_ref, *rest):
    in_refs, out_ref, rows_ref = rest[:ins], rest[ins], rest[ins + 1]
    row = 0
    for ref in in_refs:
        rows_ref[row : row + ref.shape[0], :] = ref[...].astype(jnp.float32)
        row += ref.shape[0]
    ordered = jnp.dot(arrange_ref[...], rows_ref[...].astype(jnp.bfloat16), preferred_element_type=jnp.float32)
    out_ref[...] = (ordered * gain_ref[0]).astype(jnp.bfloat16).reshape(out_ref.shape)


def place_call(gain, arrange, pieces, lines):
    cols = pieces[0].shape[1]
    block = PLACE_TILES * LANES
    return pl.pallas_call(
        functools.partial(place_body, len(pieces)),
        grid=(cols // block,),
        in_specs=[
            pl.BlockSpec(memory_space=pltpu.SMEM),
            pl.BlockSpec(arrange.shape, lambda i: (0, 0)),
        ]
        + [pl.BlockSpec((piece.shape[0], block), lambda i: (0, i)) for piece in pieces],
        out_specs=pl.BlockSpec((2, lines, block), lambda i: (0, 0, i)),
        out_shape=jax.ShapeDtypeStruct((2, lines, cols), jnp.bfloat16),
        scratch_shapes=[pltpu.VMEM((2 * lines, block), jnp.float32)],
        name="place_lines",
    )(gain, arrange, *pieces)


def shards(
    secondary, line_valid, first_valid, last_valid, az_coef, az_base, rg_base, rg_coef, block_dest
):
    lines, cols = secondary.shape[1:]
    devices = lax.axis_size("az")
    chips = devices // 2
    half = chips // 2
    me = lax.axis_index("az")
    chip, core = me // 2, me % 2
    pos = jnp.stack([chip, core]).astype(jnp.int32)
    sibling = [(i, i ^ 1) for i in range(devices)]
    order = shift_list(chips)

    sib = lax.ppermute(secondary, "az", sibling)
    meta, edge = prepare_call(
        pos, secondary, az_coef, az_base, rg_base, block_dest, line_valid, first_valid, last_valid
    )
    across = [(2 * z + 1, 2 * z + 2) for z in range(chips - 1)] + [(2 * z + 2, 2 * z + 1) for z in range(chips - 1)]
    along = [(2 * z + 1, 2 * z + 3) for z in range(chips - 1)] + [(2 * z + 2, 2 * z) for z in range(chips - 1)]
    near = lax.ppermute(edge, "az", across)
    far = lax.ppermute(edge, "az", along)
    meta_sib = lax.ppermute(meta, "az", sibling)
    table = table_call(rg_coef, cols)

    rows = [4] * (len(order) + 1) + [2, 2]
    *made, power = filter_call(chips, pos, meta, meta_sib, secondary, sib, near, far, table, rows)

    up = lax.ppermute(made[-2], "az", chip_pairs(chips, half // 2))
    down = lax.ppermute(made[-1], "az", chip_pairs(chips, -(half // 2)))
    arrived = []
    for at, shift in enumerate(order):
        arrived.append(lax.ppermute(made[at + 1], "az", chip_pairs(chips, shift)))
    up, power, valid, first, last, dest = lax.optimization_barrier(
        (up, power, line_valid, first_valid, last_valid, block_dest)
    )
    up = lax.ppermute(up, "az", chip_pairs(chips, half - half // 2))
    down = lax.ppermute(down, "az", chip_pairs(chips, -(half - half // 2)))

    spans = jnp.maximum(last - first, 0)
    own_count = jnp.sum(jnp.where(valid > 0, spans, 0)).astype(jnp.float32)
    target = jnp.arange(devices, dtype=jnp.int32)[:, None]
    to_each = jnp.sum(jnp.where((dest // lines)[None] == target, (dest % lines)[None], 0), axis=1)
    sums = jnp.stack(
        [jnp.broadcast_to(power, (devices,)), jnp.broadcast_to(own_count, (devices,)), to_each.astype(jnp.float32)],
        axis=1,
    )
    gathered = lax.all_to_all(sums, "az", split_axis=0, concat_axis=0, tiled=True)
    totals = jnp.sum(gathered[:, :2], axis=0)
    total_power, total_count = totals[0], totals[1]
    mean_power = total_power / jnp.maximum(total_count, 1.0)
    power_gain = lax.rsqrt(mean_power + 0.5)

    shifts = jnp.array([0] + order + [half], jnp.int32)
    source_chip = (chip - shifts) % chips
    source = (2 * source_chip[:, None] + jnp.stack([core, 1 - core])[None]).reshape(-1)
    seat = jnp.sum(
        jnp.where(source[:, None] == jnp.arange(devices, dtype=jnp.int32)[None], gathered[:, 2][None], 0.0), axis=1
    )
    spot = jnp.repeat(seat, 2)[None] + jnp.tile(jnp.arange(2, dtype=jnp.float32) * lines, lines)[None]
    arrange = (spot == jnp.arange(2 * lines, dtype=jnp.float32)[:, None]).astype(jnp.bfloat16)
    coregistered = place_call(power_gain.reshape(1), arrange, [made[0]] + arrived + [up, down], lines)
    valid_share = total_count / float(cols * lines * devices)
    return (coregistered, mean_power.reshape(1), valid_share.reshape(1))


def solution(mesh):
    placed = (
        P(None, ("scene", "az"), None),
        P(("scene", "az")),
        P(("scene", "az")),
        P(("scene", "az")),
        P(None, ("scene", "az")),
        P(("scene", "az")),
        P(("scene", "az")),
        P("scene"),
        P(("scene", "az")),
    )
    return jax.shard_map(
        shards,
        mesh=mesh,
        in_specs=placed,
        out_specs=(P(None, ("scene", "az"), None), P("scene"), P("scene")),
        check_vma=False,
    )
```

```python
import functools
import math

import jax
import jax.numpy as jnp
from jax import lax
from jax.experimental import pallas as pl
from jax.experimental.pallas import tpu as pltpu
from jax.sharding import PartitionSpec as P


EDGE = 8
TAPS = 9
LANES = 128
PAIR = 2 * LANES
MAIN_TILES = 24
UNROLL = 8
TABLE_TILES = 8
PLACE_TILES = 32
EDGE_CHUNKS = 8
AHEAD = 8


def sinc_taper(distance):
    in_reach = jnp.abs(distance) < 4.0
    turn = jnp.pi * distance
    ratio = jnp.where(distance == 0.0, 1.0, jnp.sin(turn) / jnp.where(distance == 0.0, 1.0, turn))
    shaped = ratio * (0.5 + 0.5 * jnp.cos(jnp.pi * distance / 4.0))
    return jnp.where(in_reach, shaped, jnp.zeros_like(distance))


def shift_list(chips):
    half = chips // 2
    rising = [k for k in (3, 5, 8, 15, 11) if k < half]
    falling = [k for k in range(half - 1, 0, -1) if k not in rising]
    return [s * k for k in rising + falling for s in (1, -1)]


def chip_pairs(chips, shift):
    return [(2 * z + c, 2 * ((z + shift) % chips) + c) for z in range(chips) for c in range(2)]


def prepare_body(
    pos_ref, lines_ref, coef_ref, az_ref, rg_ref, dest_ref, valid_ref, first_ref, last_ref, meta_ref, edge_ref
):
    cols = lines_ref.shape[2]
    count = dest_ref.shape[1]
    low = jnp.where(valid_ref[...] > 0, first_ref[...], 2 * cols)
    high = last_ref[...]
    meta_ref[...] = jnp.zeros(meta_ref.shape, jnp.float32)
    meta_ref[0:3, :] = coef_ref[...]
    for row, value in enumerate((az_ref[...], rg_ref[...], dest_ref[...], low, high)):
        meta_ref[3 + row : 4 + row, :] = value.astype(jnp.float32)
    begin = pos_ref[1] * (count - EDGE)
    here = lax.broadcasted_iota(jnp.int32, (EDGE, count), 1) == lax.broadcasted_iota(jnp.int32, (EDGE, count), 0) + begin

    def upright(values):
        spread = jnp.where(here, values.astype(jnp.float32), 0.0)
        return jnp.sum(spread, axis=1, keepdims=True).astype(jnp.int32)

    low_at, high_at = upright(low), upright(high)
    width = cols // EDGE_CHUNKS
    for chunk in range(EDGE_CHUNKS):
        at = slice(chunk * width, (chunk + 1) * width)
        column = lax.broadcasted_iota(jnp.int32, (EDGE, width), 1) + chunk * width
        keep = (column >= low_at) & (column < high_at)
        for part in range(2):
            edge_ref[part, :, at] = jnp.where(keep, lines_ref[part, :, at].astype(jnp.float32), 0.0).astype(jnp.bfloat16)


def prepare_call(pos, secondary, az_coef, *vectors):
    lines, cols = secondary.shape[1:]
    flat = pl.BlockSpec((1, lines), lambda i, pos: (0, 0))
    return pl.pallas_call(
        prepare_body,
        grid_spec=pltpu.PrefetchScalarGridSpec(
            num_scalar_prefetch=1,
            grid=(1,),
            in_specs=[
                pl.BlockSpec((2, EDGE, cols), lambda i, pos: (0, pos[1] * (lines // EDGE - 1), 0)),
                pl.BlockSpec((3, lines), lambda i, pos: (0, 0)),
            ]
            + [flat] * len(vectors),
            out_specs=[
                pl.BlockSpec((16, lines), lambda i, pos: (0, 0)),
                pl.BlockSpec((2, EDGE, cols), lambda i, pos: (0, 0, 0)),
            ],
        ),
        out_shape=[
            jax.ShapeDtypeStruct((16, lines), jnp.float32),
            jax.ShapeDtypeStruct((2, EDGE, cols), jnp.bfloat16),
        ],
        name="prepare",
    )(pos, secondary, az_coef, *[v.reshape(1, lines) for v in vectors])


def table_body(cols, coef_ref, out_ref, taps_ref, whole_ref):
    step = pl.program_id(0)
    tiles = cols // LANES

    @pl.when(step == 0)
    def _():
        shape = (tiles, LANES)
        column = lax.broadcasted_iota(jnp.int32, shape, 0) * LANES + lax.broadcasted_iota(jnp.int32, shape, 1)
        v = (column.astype(jnp.float32) + 0.5) / cols
        offsets = coef_ref[0] + coef_ref[1] * v + coef_ref[2] * v * v + coef_ref[3] * v * v * v
        whole = jnp.round(offsets)
        part = offsets - whole
        whole_ref[...] = whole
        sine = jnp.sin(jnp.pi * part)
        cosine4 = jnp.cos(jnp.pi / 4.0 * part)
        sine4 = jnp.sin(jnp.pi / 4.0 * part)
        for k in range(TAPS):
            m = k - 4
            x = m - part
            turn = jnp.pi * x
            lifted = sine if m % 2 else -sine
            ratio = jnp.where(x == 0.0, 1.0, lifted / jnp.where(x == 0.0, 1.0, turn))
            taper = 0.5 + 0.5 * (math.cos(math.pi * m / 4) * cosine4 + math.sin(math.pi * m / 4) * sine4)
            value = jnp.where(jnp.abs(x) < 4.0, ratio * taper, 0.0)
            taps_ref[k] = value

    gap = (lax.broadcasted_iota(jnp.int32, (16, LANES), 0) - lax.broadcasted_iota(jnp.int32, (16, LANES), 1)).astype(jnp.float32)
    blank = jnp.zeros((16, LANES), jnp.bfloat16)
    pieces = [(16 * g, 16 * g) for g in range(8)] + [(LANES, LANES), (2 * LANES - 16, -16)]
    for tile in range(TABLE_TILES):
        at = pl.ds(step * TABLE_TILES + tile, 1)
        near = (gap - whole_ref[at, :]).astype(jnp.bfloat16)
        taps = [jnp.broadcast_to(taps_ref[k, at, :], (16, LANES)).astype(jnp.bfloat16) for k in range(TAPS)]
        for row, distance in pieces:
            total = blank
            for k in range(TAPS):
                total = jnp.where(near == jnp.bfloat16(k - 4 - distance), taps[k], total)
            out_ref[tile, row : row + 16, :] = total
        for g in range(1, 7):
            out_ref[tile, LANES + 16 * g : LANES + 16 * g + 16, :] = blank


def table_call(coef, cols):
    tiles = cols // LANES
    return pl.pallas_call(
        functools.partial(table_body, cols),
        grid=(tiles // TABLE_TILES,),
        in_specs=[pl.BlockSpec(memory_space=pltpu.SMEM)],
        out_specs=pl.BlockSpec((TABLE_TILES, PAIR, LANES), lambda i: (i, 0, 0)),
        out_shape=jax.ShapeDtypeStruct((tiles, PAIR, LANES), jnp.bfloat16),
        scratch_shapes=[pltpu.VMEM((TAPS, tiles, LANES), jnp.float32), pltpu.VMEM((tiles, LANES), jnp.float32)],
        name="range_table",
    )(coef)


def plan(chips, shifts, pos_ref, meta_ref, meta_sib_ref, lhs_ref, lhs_edge_ref, marks_ref, moves_ref):
    chip, core = pos_ref[0], pos_ref[1]
    lines = meta_ref.shape[1]
    count = 2 * lines
    rows = 4 * len(shifts)
    row = lax.broadcasted_iota(jnp.int32, (rows, lines), 0)
    turn = row // 4
    shift = jnp.zeros(turn.shape, jnp.int32)
    for at, distance in enumerate(shifts):
        shift = jnp.where(turn == at, distance, shift)
    goal = chip + shift
    goal = 2 * jnp.where(goal < 0, goal + chips, jnp.where(goal >= chips, goal - chips, goal)) + core
    from_sib = (row // 2) % 2 == 1
    tap = lax.broadcasted_iota(jnp.int32, (16, lines), 0)
    along = lax.broadcasted_iota(jnp.int32, (16, lines), 1)
    picked = None
    for source, (ref, home) in enumerate(((meta_ref, core), (meta_sib_ref, 1 - core))):
        fraction = ref[0:1, :] + ref[1:2, :] * 0.5 + ref[2:3, :] * 0.5 * 0.5
        features = sinc_taper((tap - 4).astype(jnp.float32) - fraction)
        start = (along + home * lines - 4).astype(jnp.float32) + ref[3:4, :]
        features = jnp.where(tap < TAPS, features, jnp.where(tap == TAPS, start, ref[4:5, :]))
        owner = ref[5:6, :].astype(jnp.int32) // lines
        chosen = (owner == goal) & (from_sib if source else ~from_sib)
        found = lax.dot_general(
            jnp.where(chosen, 1.0, 0.0).astype(jnp.bfloat16),
            features.astype(jnp.bfloat16),
            (((1,), (1,)), ((), ())),
            preferred_element_type=jnp.float32,
        )
        picked = found if picked is None else picked + found
    begin = picked[:, TAPS : TAPS + 1]

    def band(coordinate, part):
        row_part = lax.broadcasted_iota(jnp.int32, part.shape, 0) % 2
        step = jnp.where(part == row_part, coordinate.astype(jnp.float32) - begin, -1.0)
        total = jnp.zeros(step.shape, jnp.float32)
        for k in range(TAPS):
            total = jnp.where(step == k, picked[:, k : k + 1], total)
        return total.astype(jnp.bfloat16)

    lane = lax.broadcasted_iota(jnp.int32, (rows, count), 1)
    lhs_ref[:, 0:count] = band(lane % lines + core * lines, lane // lines)
    lhs_ref[:, count : 2 * count] = band(lane % lines + (1 - core) * lines, lane // lines)
    slot = lax.broadcasted_iota(jnp.int32, (rows, 4 * EDGE), 1)
    high = (slot // (2 * EDGE) + core) % 2 == 1
    coordinate = slot % EDGE + jnp.where(high, 2 * lines, -EDGE)
    lhs_edge_ref[...] = band(coordinate, slot // EDGE % 2)

    line = lax.broadcasted_iota(jnp.int32, (count, lines), 1)
    level = line == lax.broadcasted_iota(jnp.int32, (count, lines), 0) % lines
    for at, (ref, which) in enumerate(((meta_ref, 6), (meta_ref, 7), (meta_sib_ref, 6), (meta_sib_ref, 7))):
        upright = jnp.sum(jnp.where(level, ref[which : which + 1, :], 0.0), axis=1, keepdims=True)
        marks_ref[at] = jnp.broadcast_to(upright, (count, LANES)).astype(jnp.int32)
    moves_ref[...] = jnp.broadcast_to(picked[:, TAPS + 1 : TAPS + 2], (rows, LANES)).astype(jnp.int32)


def filter_body(
    chips, shifts, steps, outs, pos_ref, meta_ref, meta_sib_ref, own_ref, sib_ref, near_ref, far_ref, table_ref, *rest
):
    out_refs, power_ref = rest[:outs], rest[outs]
    turned_ref, lhs_ref, lhs_edge_ref, marks_ref, moves_ref, squares_ref = rest[outs + 1 :]
    step = pl.program_id(0)
    lines = own_ref.shape[1]
    count = 2 * lines
    tiles = steps * MAIN_TILES

    @pl.when(step == 0)
    def _():
        plan(chips, shifts, pos_ref, meta_ref, meta_sib_ref, lhs_ref, lhs_edge_ref, marks_ref, moves_ref)
        zeros = jnp.zeros(squares_ref.shape, jnp.float32)
        for row in (0, 1, tiles + 2, tiles + 3):
            turned_ref[row] = zeros
        squares_ref[...] = zeros

    lane = lax.broadcasted_iota(jnp.int32, (count, LANES), 1)
    row_lane = lax.broadcasted_iota(jnp.int32, moves_ref.shape, 1)
    source = row_lane + moves_ref[...]
    before = source < 0
    after = source >= LANES
    wrapped = source & (LANES - 1)

    @pl.when(step < steps)
    def _():
        def run(turn, _):
            for pair in range(UNROLL // 2):
                tile = turn * UNROLL + 2 * pair
                here = step * MAIN_TILES + tile
                both = pl.ds(pl.multiple_of(tile * LANES, PAIR), PAIR)

                def kept(ref, low, high):
                    values = ref[:, :, both].reshape(count, PAIR).astype(jnp.float32)
                    halves = []
                    for half in range(2):
                        column = lane + (here + half) * LANES
                        inside = (column >= marks_ref[low]) & (column < marks_ref[high])
                        value = values[:, half * LANES : (half + 1) * LANES]
                        halves.append(jnp.where(inside, value, 0.0).astype(jnp.bfloat16))
                    return jnp.concatenate(halves, axis=1)

                data = jnp.concatenate([kept(own_ref, 0, 1), kept(sib_ref, 2, 3)], axis=0)
                edges = jnp.concatenate(
                    [near_ref[:, :, both].reshape(2 * EDGE, PAIR), far_ref[:, :, both].reshape(2 * EDGE, PAIR)], axis=0
                )
                summed = jnp.dot(lhs_ref[...], data, preferred_element_type=jnp.float32)
                summed += jnp.dot(lhs_edge_ref[...], edges, preferred_element_type=jnp.float32)
                rounded = summed.astype(jnp.bfloat16).astype(jnp.float32)
                for half in range(2):
                    turned_ref[here + half + 2] = jnp.take_along_axis(
                        rounded[:, half * LANES : (half + 1) * LANES], wrapped, axis=1, mode="promise_in_bounds"
                    )
            return None

        lax.fori_loop(0, MAIN_TILES // UNROLL, run, None)

    def move(tile):
        here = jnp.where(before, turned_ref[tile + 1], jnp.where(after, turned_ref[tile + 3], turned_ref[tile + 2]))
        return jnp.where((tile >= 0) & (tile < tiles), here, 0.0)

    @pl.when(step > 0)
    def _():
        left = row_lane < LANES // 2
        first = (step - 1) * MAIN_TILES

        def run(turn, carry):
            squares, previous, middle = carry
            for inner in range(UNROLL):
                tile = turn * UNROLL + inner
                at = pl.ds(pl.multiple_of(tile * LANES, LANES), LANES)
                following = move(first + tile + 1)
                window = jnp.concatenate([middle, jnp.where(left, following, previous)], axis=1).astype(jnp.bfloat16)
                done = jnp.dot(window, table_ref[tile], preferred_element_type=jnp.float32).astype(jnp.bfloat16)
                wide = done.astype(jnp.float32)
                squares += wide * wide
                row = 0
                for ref in out_refs:
                    ref[:, at] = wide[row : row + ref.shape[0]].astype(jnp.bfloat16)
                    row += ref.shape[0]
                previous, middle = middle, following
            return squares, previous, middle

        start = (squares_ref[...], move(first - 1), move(first))
        squares_ref[...] = lax.fori_loop(0, MAIN_TILES // UNROLL, run, start)[0]

    @pl.when(step == steps)
    def _():
        power_ref[0] = jnp.sum(squares_ref[...])


def filter_call(chips, shifts, pos, meta, meta_sib, own, sib, near, far, table, row_counts):
    lines, cols = own.shape[1:]
    count = 2 * lines
    made = sum(row_counts)
    tiles = cols // LANES
    steps = tiles // MAIN_TILES
    block = MAIN_TILES * LANES

    def incoming(i):
        return (0, 0, jnp.minimum(i, steps - 1))

    def outgoing(i):
        return (0, jnp.maximum(i - 1, 0))

    smem = pl.BlockSpec(memory_space=pltpu.SMEM)
    return pl.pallas_call(
        functools.partial(filter_body, chips, shifts, steps, len(row_counts)),
        grid=(steps + 1,),
        in_specs=[
            smem,
            pl.BlockSpec(meta.shape, lambda i: (0, 0)),
            pl.BlockSpec(meta.shape, lambda i: (0, 0)),
            pl.BlockSpec((2, lines, block), incoming),
            pl.BlockSpec((2, lines, block), incoming),
            pl.BlockSpec((2, EDGE, block), incoming),
            pl.BlockSpec((2, EDGE, block), incoming),
            pl.BlockSpec((MAIN_TILES, PAIR, LANES), lambda i: (jnp.maximum(i - 1, 0), 0, 0)),
        ],
        out_specs=[pl.BlockSpec((rows, block), outgoing) for rows in row_counts] + [smem],
        out_shape=[jax.ShapeDtypeStruct((rows, cols), jnp.bfloat16) for rows in row_counts]
        + [jax.ShapeDtypeStruct((1,), jnp.float32)],
        scratch_shapes=[
            pltpu.VMEM((tiles + 4, made, LANES), jnp.float32),
            pltpu.VMEM((made, 2 * count), jnp.bfloat16),
            pltpu.VMEM((made, 4 * EDGE), jnp.bfloat16),
            pltpu.VMEM((4, count, LANES), jnp.int32),
            pltpu.VMEM((made, LANES), jnp.int32),
            pltpu.VMEM((made, LANES), jnp.float32),
        ],
        name="line_filter",
    )(pos, meta, meta_sib, own, sib, near, far, table)


def place_body(ins, gain_ref, arrange_ref, *rest):
    in_refs, out_ref, rows_ref = rest[:ins], rest[ins], rest[ins + 1]
    row = 0
    for ref in in_refs:
        rows_ref[row : row + ref.shape[0], :] = ref[...].astype(jnp.float32)
        row += ref.shape[0]
    ordered = jnp.dot(arrange_ref[...], rows_ref[...].astype(jnp.bfloat16), preferred_element_type=jnp.float32)
    out_ref[...] = (ordered * gain_ref[0]).astype(jnp.bfloat16).reshape(out_ref.shape)


def place_call(gain, arrange, pieces, lines):
    cols = pieces[0].shape[1]
    block = PLACE_TILES * LANES
    return pl.pallas_call(
        functools.partial(place_body, len(pieces)),
        grid=(cols // block,),
        in_specs=[
            pl.BlockSpec(memory_space=pltpu.SMEM),
            pl.BlockSpec(arrange.shape, lambda i: (0, 0)),
        ]
        + [pl.BlockSpec((piece.shape[0], block), lambda i: (0, i)) for piece in pieces],
        out_specs=pl.BlockSpec((2, lines, block), lambda i: (0, 0, i)),
        out_shape=jax.ShapeDtypeStruct((2, lines, cols), jnp.bfloat16),
        scratch_shapes=[pltpu.VMEM((2 * lines, block), jnp.float32)],
        name="place_lines",
    )(gain, arrange, *pieces)


def shards(
    secondary, line_valid, first_valid, last_valid, az_coef, az_base, rg_base, rg_coef, block_dest
):
    lines, cols = secondary.shape[1:]
    devices = lax.axis_size("az")
    chips = devices // 2
    half = chips // 2
    me = lax.axis_index("az")
    chip, core = me // 2, me % 2
    pos = jnp.stack([chip, core]).astype(jnp.int32)
    sibling = [(i, i ^ 1) for i in range(devices)]
    order = shift_list(chips)

    sib = lax.ppermute(secondary, "az", sibling)
    meta, edge = prepare_call(
        pos, secondary, az_coef, az_base, rg_base, block_dest, line_valid, first_valid, last_valid
    )
    across = [(2 * z + 1, 2 * z + 2) for z in range(chips - 1)] + [(2 * z + 2, 2 * z + 1) for z in range(chips - 1)]
    along = [(2 * z + 1, 2 * z + 3) for z in range(chips - 1)] + [(2 * z + 2, 2 * z) for z in range(chips - 1)]
    near = lax.ppermute(edge, "az", across)
    far = lax.ppermute(edge, "az", along)
    meta_sib = lax.ppermute(meta, "az", sibling)
    coef, sib = lax.optimization_barrier((rg_coef, sib))
    table = table_call(coef, cols)

    inputs = (pos, meta, meta_sib, secondary, sib, near, far, table)
    ahead, behind = order[:AHEAD], [0] + order[AHEAD:] + [half]
    *made_ahead, power_ahead = filter_call(chips, ahead, *inputs, [4] * AHEAD)
    *made, power = filter_call(chips, behind, *inputs, [4] * (len(behind) - 1) + [2, 2])
    made = made[:1] + made_ahead + made[1:]

    up = lax.ppermute(made[-2], "az", chip_pairs(chips, half // 2))
    down = lax.ppermute(made[-1], "az", chip_pairs(chips, -(half // 2)))
    arrived = []
    for at, shift in enumerate(order):
        arrived.append(lax.ppermute(made[at + 1], "az", chip_pairs(chips, shift)))
    arrived[0], power, valid, first, last, dest = lax.optimization_barrier(
        (arrived[0], power + power_ahead, line_valid, first_valid, last_valid, block_dest)
    )
    up = lax.ppermute(up, "az", chip_pairs(chips, half - half // 2))
    down = lax.ppermute(down, "az", chip_pairs(chips, -(half - half // 2)))

    spans = jnp.maximum(last - first, 0)
    own_count = jnp.sum(jnp.where(valid > 0, spans, 0)).astype(jnp.float32)
    target = jnp.arange(devices, dtype=jnp.int32)[:, None]
    to_each = jnp.sum(jnp.where((dest // lines)[None] == target, (dest % lines)[None], 0), axis=1)
    sums = jnp.stack(
        [jnp.broadcast_to(power, (devices,)), jnp.broadcast_to(own_count, (devices,)), to_each.astype(jnp.float32)],
        axis=1,
    )
    gathered = lax.all_to_all(sums, "az", split_axis=0, concat_axis=0, tiled=True)
    totals = jnp.sum(gathered[:, :2], axis=0)
    total_power, total_count = totals[0], totals[1]
    mean_power = total_power / jnp.maximum(total_count, 1.0)
    power_gain = lax.rsqrt(mean_power + 0.5)

    chip, core, _ = lax.optimization_barrier((chip, core, gathered))
    shifts = jnp.array([0] + order + [half], jnp.int32)
    source_chip = (chip - shifts) % chips
    source = (2 * source_chip[:, None] + jnp.stack([core, 1 - core])[None]).reshape(-1)
    seat = jnp.sum(
        jnp.where(source[:, None] == jnp.arange(devices, dtype=jnp.int32)[None], gathered[:, 2][None], 0.0), axis=1
    )
    spot = jnp.repeat(seat, 2)[None] + jnp.tile(jnp.arange(2, dtype=jnp.float32) * lines, lines)[None]
    arrange = (spot == jnp.arange(2 * lines, dtype=jnp.float32)[:, None]).astype(jnp.bfloat16)
    coregistered = place_call(power_gain.reshape(1), arrange, [made[0]] + arrived + [up, down], lines)
    valid_share = total_count / float(cols * lines * devices)
    return (coregistered, mean_power.reshape(1), valid_share.reshape(1))


def solution(mesh):
    placed = (
        P(None, ("scene", "az"), None),
        P(("scene", "az")),
        P(("scene", "az")),
        P(("scene", "az")),
        P(None, ("scene", "az")),
        P(("scene", "az")),
        P(("scene", "az")),
        P("scene"),
        P(("scene", "az")),
    )
    return jax.shard_map(
        shards,
        mesh=mesh,
        in_specs=placed,
        out_specs=(P(None, ("scene", "az"), None), P("scene"), P("scene")),
        check_vma=False,
    )
```

```python
import functools
import math

import jax
import jax.numpy as jnp
from jax import lax
from jax.experimental import pallas as pl
from jax.experimental.pallas import tpu as pltpu
from jax.sharding import PartitionSpec as P


EDGE = 8
TAPS = 9
LANES = 128
PAIR = 2 * LANES
MAIN_TILES = 24
UNROLL = 8
TABLE_TILES = 8
PLACE_TILES = 48
EDGE_CHUNKS = 8


def sinc_taper(distance):
    in_reach = jnp.abs(distance) < 4.0
    turn = jnp.pi * distance
    ratio = jnp.where(distance == 0.0, 1.0, jnp.sin(turn) / jnp.where(distance == 0.0, 1.0, turn))
    shaped = ratio * (0.5 + 0.5 * jnp.cos(jnp.pi * distance / 4.0))
    return jnp.where(in_reach, shaped, jnp.zeros_like(distance))


def shift_list(chips):
    half = chips // 2
    rising = [k for k in (2, 3, 5, 8, 11, 15) if k < half]
    falling = [k for k in range(half - 1, 0, -1) if k not in rising]
    return [s * k for k in rising + falling for s in (1, -1)]


def chip_pairs(chips, shift):
    return [(2 * z + c, 2 * ((z + shift) % chips) + c) for z in range(chips) for c in range(2)]


def prepare_body(
    pos_ref, lines_ref, coef_ref, az_ref, rg_ref, dest_ref, valid_ref, first_ref, last_ref, meta_ref, edge_ref
):
    cols = lines_ref.shape[2]
    count = dest_ref.shape[1]
    low = jnp.where(valid_ref[...] > 0, first_ref[...], 2 * cols)
    high = last_ref[...]
    meta_ref[...] = jnp.zeros(meta_ref.shape, jnp.float32)
    meta_ref[0:3, :] = coef_ref[...]
    for row, value in enumerate((az_ref[...], rg_ref[...], dest_ref[...], low, high)):
        meta_ref[3 + row : 4 + row, :] = value.astype(jnp.float32)
    begin = pos_ref[1] * (count - EDGE)
    here = lax.broadcasted_iota(jnp.int32, (EDGE, count), 1) == lax.broadcasted_iota(jnp.int32, (EDGE, count), 0) + begin

    def upright(values):
        spread = jnp.where(here, values.astype(jnp.float32), 0.0)
        return jnp.sum(spread, axis=1, keepdims=True).astype(jnp.int32)

    low_at, high_at = upright(low), upright(high)
    width = cols // EDGE_CHUNKS
    for chunk in range(EDGE_CHUNKS):
        at = slice(chunk * width, (chunk + 1) * width)
        column = lax.broadcasted_iota(jnp.int32, (EDGE, width), 1) + chunk * width
        keep = (column >= low_at) & (column < high_at)
        for part in range(2):
            edge_ref[part, :, at] = jnp.where(keep, lines_ref[part, :, at].astype(jnp.float32), 0.0).astype(jnp.bfloat16)


def prepare_call(pos, secondary, az_coef, *vectors):
    lines, cols = secondary.shape[1:]
    flat = pl.BlockSpec((1, lines), lambda i, pos: (0, 0))
    return pl.pallas_call(
        prepare_body,
        grid_spec=pltpu.PrefetchScalarGridSpec(
            num_scalar_prefetch=1,
            grid=(1,),
            in_specs=[
                pl.BlockSpec((2, EDGE, cols), lambda i, pos: (0, pos[1] * (lines // EDGE - 1), 0)),
                pl.BlockSpec((3, lines), lambda i, pos: (0, 0)),
            ]
            + [flat] * len(vectors),
            out_specs=[
                pl.BlockSpec((16, lines), lambda i, pos: (0, 0)),
                pl.BlockSpec((2, EDGE, cols), lambda i, pos: (0, 0, 0)),
            ],
        ),
        out_shape=[
            jax.ShapeDtypeStruct((16, lines), jnp.float32),
            jax.ShapeDtypeStruct((2, EDGE, cols), jnp.bfloat16),
        ],
        name="prepare",
    )(pos, secondary, az_coef, *[v.reshape(1, lines) for v in vectors])


def table_body(cols, coef_ref, out_ref, taps_ref, whole_ref):
    step = pl.program_id(0)
    tiles = cols // LANES

    @pl.when(step == 0)
    def _():
        shape = (tiles, LANES)
        column = lax.broadcasted_iota(jnp.int32, shape, 0) * LANES + lax.broadcasted_iota(jnp.int32, shape, 1)
        v = (column.astype(jnp.float32) + 0.5) / cols
        offsets = coef_ref[0] + coef_ref[1] * v + coef_ref[2] * v * v + coef_ref[3] * v * v * v
        whole = jnp.round(offsets)
        part = offsets - whole
        whole_ref[...] = whole
        sine = jnp.sin(jnp.pi * part)
        cosine4 = jnp.cos(jnp.pi / 4.0 * part)
        sine4 = jnp.sin(jnp.pi / 4.0 * part)
        for k in range(TAPS):
            m = k - 4
            x = m - part
            turn = jnp.pi * x
            lifted = sine if m % 2 else -sine
            ratio = jnp.where(x == 0.0, 1.0, lifted / jnp.where(x == 0.0, 1.0, turn))
            taper = 0.5 + 0.5 * (math.cos(math.pi * m / 4) * cosine4 + math.sin(math.pi * m / 4) * sine4)
            value = jnp.where(jnp.abs(x) < 4.0, ratio * taper, 0.0)
            taps_ref[k] = value

    gap = (lax.broadcasted_iota(jnp.int32, (16, LANES), 0) - lax.broadcasted_iota(jnp.int32, (16, LANES), 1)).astype(jnp.float32)
    blank = jnp.zeros((16, LANES), jnp.bfloat16)
    pieces = [(16 * g, 16 * g) for g in range(8)] + [(LANES, LANES), (2 * LANES - 16, -16)]
    for tile in range(TABLE_TILES):
        at = pl.ds(step * TABLE_TILES + tile, 1)
        near = (gap - whole_ref[at, :]).astype(jnp.bfloat16)
        taps = [jnp.broadcast_to(taps_ref[k, at, :], (16, LANES)).astype(jnp.bfloat16) for k in range(TAPS)]
        for row, distance in pieces:
            total = blank
            for k in range(TAPS):
                total = jnp.where(near == jnp.bfloat16(k - 4 - distance), taps[k], total)
            out_ref[tile, row : row + 16, :] = total
        for g in range(1, 7):
            out_ref[tile, LANES + 16 * g : LANES + 16 * g + 16, :] = blank


def table_call(coef, cols):
    tiles = cols // LANES
    return pl.pallas_call(
        functools.partial(table_body, cols),
        grid=(tiles // TABLE_TILES,),
        in_specs=[pl.BlockSpec(memory_space=pltpu.SMEM)],
        out_specs=pl.BlockSpec((TABLE_TILES, PAIR, LANES), lambda i: (i, 0, 0)),
        out_shape=jax.ShapeDtypeStruct((tiles, PAIR, LANES), jnp.bfloat16),
        scratch_shapes=[pltpu.VMEM((TAPS, tiles, LANES), jnp.float32), pltpu.VMEM((tiles, LANES), jnp.float32)],
        name="range_table",
    )(coef)


def plan(chips, pos_ref, meta_ref, meta_sib_ref, lhs_ref, lhs_edge_ref, marks_ref):
    chip, core = pos_ref[0], pos_ref[1]
    lines = meta_ref.shape[1]
    count = 2 * lines
    row = lax.broadcasted_iota(jnp.int32, (count, lines), 0)
    turn = row // 4
    shift = jnp.where(turn == chips - 1, chips // 2, 0)
    for at, distance in enumerate(shift_list(chips)):
        shift = jnp.where(turn == at + 1, distance, shift)
    goal = chip + shift
    goal = 2 * jnp.where(goal < 0, goal + chips, jnp.where(goal >= chips, goal - chips, goal)) + core
    from_sib = (row // 2) % 2 == 1
    line = lax.broadcasted_iota(jnp.int32, (count, lines), 1)
    tap = lax.broadcasted_iota(jnp.int32, (16, lines), 0)
    along = lax.broadcasted_iota(jnp.int32, (16, lines), 1)
    picked = None
    for source, (ref, home) in enumerate(((meta_ref, core), (meta_sib_ref, 1 - core))):
        fraction = ref[0:1, :] + ref[1:2, :] * 0.5 + ref[2:3, :] * 0.5 * 0.5
        features = sinc_taper((tap - 4).astype(jnp.float32) - fraction)
        start = (along + home * lines - 4).astype(jnp.float32) + ref[3:4, :]
        features = jnp.where(tap < TAPS, features, jnp.where(tap == TAPS, start, ref[4:5, :]))
        owner = ref[5:6, :].astype(jnp.int32) // lines
        chosen = (owner == goal) & (from_sib if source else ~from_sib)
        found = lax.dot_general(
            jnp.where(chosen, 1.0, 0.0).astype(jnp.bfloat16),
            features.astype(jnp.bfloat16),
            (((1,), (1,)), ((), ())),
            preferred_element_type=jnp.float32,
        )
        picked = found if picked is None else picked + found
    begin = picked[:, TAPS : TAPS + 1]

    def band(coordinate, part):
        row_part = lax.broadcasted_iota(jnp.int32, part.shape, 0) % 2
        step = jnp.where(part == row_part, coordinate.astype(jnp.float32) - begin, -1.0)
        total = jnp.zeros(step.shape, jnp.float32)
        for k in range(TAPS):
            total = jnp.where(step == k, picked[:, k : k + 1], total)
        return total.astype(jnp.bfloat16)

    lane = lax.broadcasted_iota(jnp.int32, (count, count), 1)
    lhs_ref[:, 0:count] = band(lane % lines + core * lines, lane // lines)
    lhs_ref[:, count : 2 * count] = band(lane % lines + (1 - core) * lines, lane // lines)
    slot = lax.broadcasted_iota(jnp.int32, (count, 4 * EDGE), 1)
    high = (slot // (2 * EDGE) + core) % 2 == 1
    coordinate = slot % EDGE + jnp.where(high, 2 * lines, -EDGE)
    lhs_edge_ref[...] = band(coordinate, slot // EDGE % 2)

    level = line == row % lines
    for at, (ref, which) in enumerate(((meta_ref, 6), (meta_ref, 7), (meta_sib_ref, 6), (meta_sib_ref, 7))):
        upright = jnp.sum(jnp.where(level, ref[which : which + 1, :], 0.0), axis=1, keepdims=True)
        marks_ref[at] = jnp.broadcast_to(upright, (count, LANES)).astype(jnp.int32)
    marks_ref[4] = jnp.broadcast_to(picked[:, TAPS + 1 : TAPS + 2], (count, LANES)).astype(jnp.int32)


def filter_body(
    chips, steps, outs, pos_ref, meta_ref, meta_sib_ref, own_ref, sib_ref, near_ref, far_ref, table_ref, *rest
):
    out_refs, power_ref = rest[:outs], rest[outs]
    turned_ref, lhs_ref, lhs_edge_ref, marks_ref, squares_ref = rest[outs + 1 :]
    step = pl.program_id(0)
    lines = own_ref.shape[1]
    count = 2 * lines
    tiles = steps * MAIN_TILES

    @pl.when(step == 0)
    def _():
        plan(chips, pos_ref, meta_ref, meta_sib_ref, lhs_ref, lhs_edge_ref, marks_ref)
        zeros = jnp.zeros((count, LANES), jnp.float32)
        for row in (0, 1, tiles + 2, tiles + 3):
            turned_ref[row] = zeros
        squares_ref[...] = zeros

    lane = lax.broadcasted_iota(jnp.int32, (count, LANES), 1)
    source = lane + marks_ref[4]
    before = source < 0
    after = source >= LANES
    wrapped = source & (LANES - 1)

    @pl.when(step < steps)
    def _():
        def run(turn, _):
            for pair in range(UNROLL // 2):
                tile = turn * UNROLL + 2 * pair
                here = step * MAIN_TILES + tile
                both = pl.ds(pl.multiple_of(tile * LANES, PAIR), PAIR)

                def kept(ref, low, high):
                    values = ref[:, :, both].reshape(count, PAIR).astype(jnp.float32)
                    halves = []
                    for half in range(2):
                        column = lane + (here + half) * LANES
                        inside = (column >= marks_ref[low]) & (column < marks_ref[high])
                        value = values[:, half * LANES : (half + 1) * LANES]
                        halves.append(jnp.where(inside, value, 0.0).astype(jnp.bfloat16))
                    return jnp.concatenate(halves, axis=1)

                data = jnp.concatenate([kept(own_ref, 0, 1), kept(sib_ref, 2, 3)], axis=0)
                edges = jnp.concatenate(
                    [near_ref[:, :, both].reshape(2 * EDGE, PAIR), far_ref[:, :, both].reshape(2 * EDGE, PAIR)], axis=0
                )
                summed = jnp.dot(lhs_ref[...], data, preferred_element_type=jnp.float32)
                summed += jnp.dot(lhs_edge_ref[...], edges, preferred_element_type=jnp.float32)
                rounded = summed.astype(jnp.bfloat16).astype(jnp.float32)
                for half in range(2):
                    turned_ref[here + half + 2] = jnp.take_along_axis(
                        rounded[:, half * LANES : (half + 1) * LANES], wrapped, axis=1, mode="promise_in_bounds"
                    )
            return None

        lax.fori_loop(0, MAIN_TILES // UNROLL, run, None)

    def move(tile):
        here = jnp.where(before, turned_ref[tile + 1], jnp.where(after, turned_ref[tile + 3], turned_ref[tile + 2]))
        return jnp.where((tile >= 0) & (tile < tiles), here, 0.0)

    @pl.when(step > 0)
    def _():
        left = lane < LANES // 2
        first = (step - 1) * MAIN_TILES

        def run(turn, carry):
            squares, previous, middle = carry
            for inner in range(UNROLL):
                tile = turn * UNROLL + inner
                at = pl.ds(pl.multiple_of(tile * LANES, LANES), LANES)
                following = move(first + tile + 1)
                window = jnp.concatenate([middle, jnp.where(left, following, previous)], axis=1).astype(jnp.bfloat16)
                done = jnp.dot(window, table_ref[tile], preferred_element_type=jnp.float32).astype(jnp.bfloat16)
                wide = done.astype(jnp.float32)
                squares += wide * wide
                row = 0
                for ref in out_refs:
                    ref[:, at] = wide[row : row + ref.shape[0]].astype(jnp.bfloat16)
                    row += ref.shape[0]
                previous, middle = middle, following
            return squares, previous, middle

        start = (squares_ref[...], move(first - 1), move(first))
        squares_ref[...] = lax.fori_loop(0, MAIN_TILES // UNROLL, run, start)[0]

    @pl.when(step == steps)
    def _():
        power_ref[0] = jnp.sum(squares_ref[...])


def filter_call(chips, pos, meta, meta_sib, own, sib, near, far, table, row_counts):
    lines, cols = own.shape[1:]
    count = 2 * lines
    tiles = cols // LANES
    steps = tiles // MAIN_TILES
    block = MAIN_TILES * LANES

    def incoming(i):
        return (0, 0, jnp.minimum(i, steps - 1))

    def outgoing(i):
        return (0, jnp.maximum(i - 1, 0))

    smem = pl.BlockSpec(memory_space=pltpu.SMEM)
    return pl.pallas_call(
        functools.partial(filter_body, chips, steps, len(row_counts)),
        grid=(steps + 1,),
        in_specs=[
            smem,
            pl.BlockSpec(meta.shape, lambda i: (0, 0)),
            pl.BlockSpec(meta.shape, lambda i: (0, 0)),
            pl.BlockSpec((2, lines, block), incoming),
            pl.BlockSpec((2, lines, block), incoming),
            pl.BlockSpec((2, EDGE, block), incoming),
            pl.BlockSpec((2, EDGE, block), incoming),
            pl.BlockSpec((MAIN_TILES, PAIR, LANES), lambda i: (jnp.maximum(i - 1, 0), 0, 0)),
        ],
        out_specs=[pl.BlockSpec((rows, block), outgoing) for rows in row_counts] + [smem],
        out_shape=[jax.ShapeDtypeStruct((rows, cols), jnp.bfloat16) for rows in row_counts]
        + [jax.ShapeDtypeStruct((1,), jnp.float32)],
        scratch_shapes=[
            pltpu.VMEM((tiles + 4, count, LANES), jnp.float32),
            pltpu.VMEM((count, 2 * count), jnp.bfloat16),
            pltpu.VMEM((count, 4 * EDGE), jnp.bfloat16),
            pltpu.VMEM((5, count, LANES), jnp.int32),
            pltpu.VMEM((count, LANES), jnp.float32),
        ],
        name="line_filter",
    )(pos, meta, meta_sib, own, sib, near, far, table)


def place_body(ins, gain_ref, arrange_ref, *rest):
    in_refs, out_ref, rows_ref = rest[:ins], rest[ins], rest[ins + 1]
    row = 0
    for ref in in_refs:
        rows_ref[row : row + ref.shape[0], :] = ref[...].astype(jnp.float32)
        row += ref.shape[0]
    ordered = jnp.dot(arrange_ref[...], rows_ref[...].astype(jnp.bfloat16), preferred_element_type=jnp.float32)
    out_ref[...] = (ordered * gain_ref[0]).astype(jnp.bfloat16).reshape(out_ref.shape)


def place_call(gain, arrange, pieces, lines):
    cols = pieces[0].shape[1]
    block = PLACE_TILES * LANES
    return pl.pallas_call(
        functools.partial(place_body, len(pieces)),
        grid=(cols // block,),
        in_specs=[
            pl.BlockSpec(memory_space=pltpu.SMEM),
            pl.BlockSpec(arrange.shape, lambda i: (0, 0)),
        ]
        + [pl.BlockSpec((piece.shape[0], block), lambda i: (0, i)) for piece in pieces],
        out_specs=pl.BlockSpec((2, lines, block), lambda i: (0, 0, i)),
        out_shape=jax.ShapeDtypeStruct((2, lines, cols), jnp.bfloat16),
        scratch_shapes=[pltpu.VMEM((2 * lines, block), jnp.float32)],
        name="place_lines",
    )(gain, arrange, *pieces)


def shards(
    secondary, line_valid, first_valid, last_valid, az_coef, az_base, rg_base, rg_coef, block_dest
):
    lines, cols = secondary.shape[1:]
    devices = lax.axis_size("az")
    chips = devices // 2
    half = chips // 2
    me = lax.axis_index("az")
    chip, core = me // 2, me % 2
    pos = jnp.stack([chip, core]).astype(jnp.int32)
    sibling = [(i, i ^ 1) for i in range(devices)]
    order = shift_list(chips)

    sib = lax.ppermute(secondary, "az", sibling)
    meta, edge = prepare_call(
        pos, secondary, az_coef, az_base, rg_base, block_dest, line_valid, first_valid, last_valid
    )
    across = [(2 * z + 1, 2 * z + 2) for z in range(chips - 1)] + [(2 * z + 2, 2 * z + 1) for z in range(chips - 1)]
    along = [(2 * z + 1, 2 * z + 3) for z in range(chips - 1)] + [(2 * z + 2, 2 * z) for z in range(chips - 1)]
    near = lax.ppermute(edge, "az", across)
    far = lax.ppermute(edge, "az", along)
    meta_sib = lax.ppermute(meta, "az", sibling)
    coef, sib = lax.optimization_barrier((rg_coef, sib))
    table = table_call(coef, cols)

    rows = [4] * (len(order) + 1) + [2, 2]
    *made, power = filter_call(chips, pos, meta, meta_sib, secondary, sib, near, far, table, rows)

    up = lax.ppermute(made[-2], "az", chip_pairs(chips, half // 2))
    down = lax.ppermute(made[-1], "az", chip_pairs(chips, -(half // 2)))
    arrived = []
    for at, shift in enumerate(order):
        arrived.append(lax.ppermute(made[at + 1], "az", chip_pairs(chips, shift)))
    arrived[0], power, valid, first, last, dest = lax.optimization_barrier(
        (arrived[0], power, line_valid, first_valid, last_valid, block_dest)
    )
    up = lax.ppermute(up, "az", chip_pairs(chips, half - half // 2))
    down = lax.ppermute(down, "az", chip_pairs(chips, -(half - half // 2)))

    spans = jnp.maximum(last - first, 0)
    own_count = jnp.sum(jnp.where(valid > 0, spans, 0)).astype(jnp.float32)
    target = jnp.arange(devices, dtype=jnp.int32)[:, None]
    to_each = jnp.sum(jnp.where((dest // lines)[None] == target, (dest % lines)[None], 0), axis=1)
    sums = jnp.stack(
        [jnp.broadcast_to(power, (devices,)), jnp.broadcast_to(own_count, (devices,)), to_each.astype(jnp.float32)],
        axis=1,
    )
    gathered = lax.all_to_all(sums, "az", split_axis=0, concat_axis=0, tiled=True)
    totals = jnp.sum(gathered[:, :2], axis=0)
    total_power, total_count = totals[0], totals[1]
    mean_power = total_power / jnp.maximum(total_count, 1.0)
    power_gain = lax.rsqrt(mean_power + 0.5)

    chip, core, _ = lax.optimization_barrier((chip, core, gathered))
    shifts = jnp.array([0] + order + [half], jnp.int32)
    source_chip = (chip - shifts) % chips
    source = (2 * source_chip[:, None] + jnp.stack([core, 1 - core])[None]).reshape(-1)
    seat = jnp.sum(
        jnp.where(source[:, None] == jnp.arange(devices, dtype=jnp.int32)[None], gathered[:, 2][None], 0.0), axis=1
    )
    spot = jnp.repeat(seat, 2)[None] + jnp.tile(jnp.arange(2, dtype=jnp.float32) * lines, lines)[None]
    arrange = (spot == jnp.arange(2 * lines, dtype=jnp.float32)[:, None]).astype(jnp.bfloat16)
    coregistered = place_call(power_gain.reshape(1), arrange, [made[0]] + arrived + [up, down], lines)
    valid_share = total_count / float(cols * lines * devices)
    return (coregistered, mean_power.reshape(1), valid_share.reshape(1))


def solution(mesh):
    placed = (
        P(None, ("scene", "az"), None),
        P(("scene", "az")),
        P(("scene", "az")),
        P(("scene", "az")),
        P(None, ("scene", "az")),
        P(("scene", "az")),
        P(("scene", "az")),
        P("scene"),
        P(("scene", "az")),
    )
    return jax.shard_map(
        shards,
        mesh=mesh,
        in_specs=placed,
        out_specs=(P(None, ("scene", "az"), None), P("scene"), P("scene")),
        check_vma=False,
    )
```
